256 devices in a mesh: prow: 16 (over z, core), pcol: 16 (over y, x).
Axes of the slice: x: 4, y: 4, z: 8, core: 2. Of those that a mesh axis runs over, the one named last changes fastest.
Arguments:
- matrix: float32 [16384, 24576], P('prow', 'pcol'), may hold values from -14 to 142, as said below
Outputs:
- factored: float32 [16384, 24576], P('prow', 'pcol')
- tfactors: float32 [2, 128, 128], replicated
The draws below stay inside these ranges and needn't reach their ends.
Inputs may be any that keep to these rules, and one draw needn't show every extreme that they name: `matrix`: real entries.
All inputs are finite; a program needn't handle non-finite values.
Results may differ from the reference program's by a relative error of at most 0.0003.
Values sent between devices are 32-bit elements; how exact they have to be, the bound alone decides.
No kernel may reach another device: no remote copies, remote signals or barrier semaphores. Data moves between devices by JAX's collectives and lax.ppermute only.
A program may use at most 128 MiB of HBM per device.

```python
import math
import jax
import jax.numpy as jnp
from jax import lax

NB = 128
NCOL = 24576
ROWS = 16384


def draw_matrix(key, part):
    noise_key = jax.random.fold_in(key, 11)
    base = jax.random.truncated_normal(noise_key, -6.0, 6.0, (ROWS, NCOL), jnp.float32)
    diagonal = (jnp.arange(ROWS)[:, None] == jnp.arange(NCOL)[None, :]).astype(jnp.float32)
    return base + math.sqrt(ROWS) * diagonal


def setup_inputs(seed: int = 0) -> dict:
    streams_of = jax.random.split(jax.random.key(seed), 2)
    return {
        "matrix": draw_matrix(jax.random.fold_in(streams_of[1], 71), 0),
    }


highest = lax.Precision.HIGHEST

def transposed_product(left, right):
    return lax.dot_general(left.astype(jnp.float32), right.astype(jnp.float32), (((0,), (0,)), ((), ())), precision=highest, preferred_element_type=jnp.float32)

def matmul(left, right):
    return jnp.dot(left.astype(jnp.float32), right.astype(jnp.float32), precision=highest, preferred_element_type=jnp.float32)

def householder_panel(panel_cols, first_row):
    row_count = panel_cols.shape[0]
    row_ids = jnp.arange(row_count, dtype=jnp.int32)
    column_ids = jnp.arange(NB, dtype=jnp.int32)

    def single_column(column, carry):
        current, vectors = carry
        column = column.astype(jnp.int32)
        target = (first_row + column).astype(jnp.int32)
        values = lax.dynamic_slice_in_dim(current, column, 1, 1)[:, 0]
        below = jnp.where(row_ids >= target, values, jnp.zeros_like(values))
        length = jnp.sqrt(jnp.sum(below * below))
        leading = lax.dynamic_index_in_dim(values, target, 0, keepdims=False)
        divisor = leading + length
        vector = jnp.where(row_ids == target, jnp.ones_like(below), below / divisor)
        tau_value = divisor / length
        weights = jnp.dot(vector, current, precision=highest) * (column_ids >= column).astype(current.dtype)
        current = current - tau_value * vector[:, None] * weights[None, :]
        vectors = lax.dynamic_update_slice(vectors, vector[:, None], (jnp.int32(0), column))
        return (current, vectors)
    start_vectors = jnp.zeros((row_count, NB), panel_cols.dtype)
    current, vectors = lax.fori_loop(0, NB, single_column, (panel_cols, start_vectors))
    packed_panel = jnp.where(row_ids[:, None] > first_row + column_ids[None, :], vectors, current)
    inner = transposed_product(vectors, vectors)
    inverse_t = jnp.triu(inner, 1) + jnp.diag(jnp.diag(inner)) * 0.5
    identity = jnp.eye(NB, dtype=panel_cols.dtype)
    tfactor = jax.scipy.linalg.solve_triangular(inverse_t, identity, lower=False)
    return (vectors, tfactor, packed_panel)

def reference(matrix):
    column_ids = jnp.arange(NCOL, dtype=jnp.int32)
    leading_reflector_vectors, first_t, leading_packed_panel = householder_panel(matrix[:, :NB], 0)
    first_products = transposed_product(leading_reflector_vectors, matrix)
    first_z = jnp.where((column_ids >= NB)[None, :], matmul(first_t.T, first_products), 0.0)
    second_panel = matrix[:, NB:2 * NB] - matmul(leading_reflector_vectors, first_z[:, NB:2 * NB])
    second_vectors, second_t, following_packed_panel = householder_panel(second_panel, NB)
    coupling = transposed_product(second_vectors, leading_reflector_vectors)
    second_products = transposed_product(second_vectors, matrix) - matmul(coupling, first_z)
    second_z = jnp.where((column_ids >= 2 * NB)[None, :], matmul(second_t.T, second_products), 0.0)
    both_vectors = jnp.concatenate([leading_reflector_vectors, second_vectors], axis=1)
    both_z = jnp.concatenate([first_z, second_z], axis=0)

    def one_block(index, current):
        begin = (index * NB).astype(jnp.int32)
        block_cols = lax.dynamic_slice_in_dim(current, begin, NB, 1)
        block_z = lax.dynamic_slice_in_dim(both_z, begin, NB, 1)
        return lax.dynamic_update_slice(current, block_cols - matmul(both_vectors, block_z), (jnp.int32(0), begin))
    result = lax.fori_loop(0, NCOL // NB, one_block, matrix)
    result = result.at[:, :2 * NB].set(jnp.concatenate([leading_packed_panel, following_packed_panel], axis=1))
    return (result, jnp.stack([first_t, second_t]))
```

```python
import jax
import jax.numpy as jnp
from jax import lax
from jax.experimental import pallas as pl
from jax.experimental.pallas import tpu as pltpu
from jax.sharding import PartitionSpec as P

NB = 128
WIDE = 2 * NB
STRIP = 8
LEVELS, CORES = 8, 2

f32, bf16 = jnp.float32, jnp.bfloat16


def three_parts(value):
    first = value.astype(bf16).astype(f32)
    rest = value - first
    second = rest.astype(bf16).astype(f32)
    return first, second, (rest - second).astype(bf16).astype(f32)


def strip_product(left, right):
    a, b, c = three_parts(left)
    d, e, f = three_parts(right)
    return lax.dot_general(
        jnp.concatenate([a, a, b, b, a, c], axis=0).astype(bf16),
        jnp.concatenate([d, e, d, e, f, d], axis=0).astype(bf16),
        (((0,), (0,)), ((), ())),
        preferred_element_type=f32,
    )


def strip_columns(rows, first, lanes):
    return [
        jnp.sum(jnp.where(lanes == first + c, rows, 0.0), axis=1, keepdims=True)
        for c in range(STRIP)
    ]


def identity_matrix():
    rows = lax.broadcasted_iota(jnp.int32, (WIDE, WIDE), 0)
    return (rows == lax.broadcasted_iota(jnp.int32, (WIDE, WIDE), 1)).astype(f32)


def strips_of(half):
    count = WIDE // STRIP // 2
    return half * count, (half + 1) * count


def cholesky_kernel(gram_ref, upper_ref, inverse_ref, work):
    work[:, :WIDE] = gram_ref[...]
    work[:, WIDE:] = identity_matrix()
    lanes = lax.broadcasted_iota(jnp.int32, (STRIP, WIDE), 1)
    row_ids = lax.broadcasted_iota(jnp.int32, (STRIP, WIDE), 0)
    sub_narrow = lax.broadcasted_iota(jnp.int32, (STRIP, 1), 0)
    sub_wide = lax.broadcasted_iota(jnp.int32, (STRIP, 2 * WIDE), 0)
    for half in range(2):
        low, high = half * NB, half * NB + 3 * NB

        def strip(index, carry):
            first = pl.multiple_of(index * STRIP, STRIP)
            rows = work[pl.ds(first, STRIP), :]
            diag = strip_columns(rows[:, :WIDE], first, lanes)
            for c in range(STRIP):
                inverse = lax.rsqrt(diag[c][c : c + 1])
                pivot_row = rows[c : c + 1] * inverse
                factor = jnp.where(sub_narrow > c, diag[c] * inverse, 0.0)
                for d in range(c + 1, STRIP):
                    diag[d] = diag[d] - factor * (diag[d][c : c + 1] * inverse)
                rows = jnp.where(sub_wide == c, pivot_row, rows - factor * pivot_row)
            upper_ref[pl.ds(first, STRIP), :] = jnp.where(
                lanes >= first + row_ids, rows[:, :WIDE], 0.0
            )
            inverse_ref[pl.ds(first, STRIP), :] = rows[:, WIDE:]
            left = jnp.where(lanes >= first + STRIP, rows[:, :WIDE], 0.0)[:, low:]
            work[low:, low:high] = work[low:, low:high] - strip_product(left, rows[:, low:high])
            return carry

        lax.fori_loop(*strips_of(half), strip, 0)


def lower_upper_kernel(
    square_ref, turned_ref, upper_ref, unit_ref, unit_inv_ref, upper_inv_ref, work, turned_work
):
    work[:, :WIDE] = square_ref[...]
    work[:, WIDE:] = identity_matrix()
    turned_work[:, :WIDE] = turned_ref[...]
    turned_work[:, WIDE:] = identity_matrix()
    lanes = lax.broadcasted_iota(jnp.int32, (STRIP, WIDE), 1)
    row_ids = lax.broadcasted_iota(jnp.int32, (STRIP, WIDE), 0)
    sub_narrow = lax.broadcasted_iota(jnp.int32, (STRIP, 1), 0)
    sub_wide = lax.broadcasted_iota(jnp.int32, (STRIP, 2 * WIDE), 0)
    for half in range(2):
        low, high = half * NB, half * NB + 3 * NB

        def strip(index, carry):
            first = pl.multiple_of(index * STRIP, STRIP)
            rows = work[pl.ds(first, STRIP), :]
            turned = turned_work[pl.ds(first, STRIP), :]
            diag = strip_columns(rows[:, :WIDE], first, lanes)
            diag_turned = strip_columns(turned[:, :WIDE], first, lanes)
            for c in range(STRIP):
                inverse = 1.0 / diag[c][c : c + 1]
                factor = jnp.where(sub_narrow > c, diag[c] * inverse, 0.0)
                factor_turned = jnp.where(sub_narrow > c, diag_turned[c], 0.0)
                for d in range(c + 1, STRIP):
                    diag[d] = diag[d] - factor * diag[d][c : c + 1]
                    diag_turned[d] = diag_turned[d] - factor_turned * (
                        diag_turned[d][c : c + 1] * inverse
                    )
                rows = rows - factor * rows[c : c + 1]
                pivot_row = turned[c : c + 1] * inverse
                turned = jnp.where(sub_wide == c, pivot_row, turned - factor_turned * pivot_row)
            kept = lanes >= first + row_ids
            upper_ref[pl.ds(first, STRIP), :] = jnp.where(kept, rows[:, :WIDE], 0.0)
            unit_ref[pl.ds(first, STRIP), :] = jnp.where(kept, turned[:, :WIDE], 0.0)
            unit_inv_ref[pl.ds(first, STRIP), :] = rows[:, WIDE:]
            upper_inv_ref[pl.ds(first, STRIP), :] = turned[:, WIDE:]
            after = lanes >= first + STRIP
            left = jnp.where(after, rows[:, :WIDE], 0.0)[:, low:]
            left_turned = jnp.where(after, turned[:, :WIDE], 0.0)[:, low:]
            work[low:, low:high] = work[low:, low:high] - strip_product(
                left_turned, rows[:, low:high]
            )
            turned_work[low:, low:high] = turned_work[low:, low:high] - strip_product(
                left, turned[:, low:high]
            )
            return carry

        lax.fori_loop(*strips_of(half), strip, 0)


square_shape = jax.ShapeDtypeStruct((WIDE, WIDE), f32)


def cholesky(gram):
    return pl.pallas_call(
        cholesky_kernel,
        out_shape=(square_shape,) * 2,
        scratch_shapes=[pltpu.VMEM((WIDE, 2 * WIDE), f32)],
        cost_estimate=pl.CostEstimate(
            flops=14_000_000_000, bytes_accessed=800_000, transcendentals=0
        ),
        name="cholesky",
    )(gram)


def lower_upper(square):
    return pl.pallas_call(
        lower_upper_kernel,
        out_shape=(square_shape,) * 4,
        scratch_shapes=[pltpu.VMEM((WIDE, 2 * WIDE), f32)] * 2,
        cost_estimate=pl.CostEstimate(
            flops=15_000_000_000, bytes_accessed=1_600_000, transcendentals=0
        ),
        name="lower_upper",
    )(square, square.T)


def product(left, right, precision=lax.Precision.HIGHEST):
    return jnp.dot(left, right, precision=precision, preferred_element_type=f32)


def transposed_product(left, right, precision=lax.Precision.HIGHEST):
    return lax.dot_general(
        left, right, (((0,), (0,)), ((), ())), precision=precision, preferred_element_type=f32
    )


def spread_panel(panel):
    count = lax.axis_size("pcol")
    rows, cols = panel.shape
    pieces = panel.reshape(count, rows // count, cols)
    piece = lax.all_to_all(pieces, "pcol", 0, 0)[0]
    everywhere = lax.all_to_all(jnp.broadcast_to(piece, pieces.shape), "pcol", 0, 0)
    return everywhere.reshape(rows, cols)


def small_sum(arrays):
    count = lax.axis_size("prow")
    pieces = jnp.concatenate([a.reshape(count, -1, a.shape[1]) for a in arrays], axis=1)
    piece = lax.all_to_all(pieces, "prow", 0, 0).sum(0)
    total = lax.all_gather(piece, "prow")
    return tuple(part.reshape(WIDE, WIDE) for part in jnp.split(total, len(arrays), axis=1))


def swap_cores(value):
    count = lax.axis_size("prow")
    return lax.ppermute(value, "prow", [(i, i ^ 1) for i in range(count)])


def halves(value, core):
    low, high = value[:NB], value[NB:]
    return jnp.where(core == 0, low, high), jnp.where(core == 0, high, low)


def large_sum(value, core):
    mine, other = halves(value, core)
    mine = mine + swap_cores(other)
    groups = [[2 * z + c for z in range(LEVELS)] for c in range(CORES)]
    pieces = mine.reshape(LEVELS, -1, value.shape[1])
    piece = lax.all_to_all(pieces, "prow", 0, 0, axis_index_groups=groups).sum(0)
    count = lax.axis_size("prow")
    received = [
        lax.ppermute(piece, "prow", [(i, (i + CORES * k) % count) for i in range(count)])
        for k in range(1, LEVELS)
    ]
    half = jnp.concatenate(received[::-1] + [piece], axis=0)
    return jnp.concatenate([half, swap_cores(half)], axis=0)


def rotated(value, core, level):
    step = NB // LEVELS

    def turn(half):
        return lax.dynamic_slice_in_dim(
            jnp.concatenate([half, half], axis=0), (level + 1) % LEVELS * step, NB, 0
        )

    mine, other = halves(value, core)
    return jnp.concatenate([turn(mine), turn(other)], axis=0)


def per_device(matrix):
    my_row, my_col = lax.axis_index("prow"), lax.axis_index("pcol")
    core, level = my_row % CORES, my_row // CORES
    on_top, has_panel = my_row == 0, my_col == 0
    panel = spread_panel(matrix[:, :WIDE])
    gram, top = small_sum(
        (transposed_product(panel, panel), jnp.where(on_top, panel[:WIDE], 0.0))
    )
    upper, inverse = cholesky(gram)
    square = top + upper
    shifted = jnp.concatenate(
        [jnp.where(on_top, panel[:WIDE] + upper, panel[:WIDE]), panel[WIDE:]], axis=0
    )
    high = lax.Precision.HIGH
    summed = large_sum(transposed_product(shifted, matrix, high), core)
    wy_upper, unit, unit_inv, upper_inv = lower_upper(square)
    turned = transposed_product(inverse, transposed_product(unit_inv, upper_inv))
    weights = transposed_product(rotated(turned, core, level), summed, high)
    column_ids = lax.broadcasted_iota(jnp.int32, (1, matrix.shape[1]), 1)
    replaced = has_panel & (column_ids < WIDE)
    weights = jnp.concatenate(
        [jnp.where(has_panel, -upper_inv.T, weights[:, :WIDE]), weights[:, WIDE:]], axis=1
    )
    result = jnp.where(replaced, 0.0, matrix) - product(shifted, weights, high)
    corner = result[:WIDE, :WIDE]
    above = jnp.triu(jnp.ones((WIDE, WIDE), jnp.bool_))
    corner = jnp.where(on_top & has_panel & above, -upper, corner)
    result = result.at[:WIDE, :WIDE].set(corner)
    factors = [
        product(wy_upper[s, s], product(inverse[s, s].T, unit_inv[s, s].T))
        for s in (slice(0, NB), slice(NB, WIDE))
    ]
    return (result, jnp.stack(factors))


def solution(mesh):
    placed = (P("prow", "pcol"),)
    return jax.shard_map(
        per_device, mesh=mesh, in_specs=placed, out_specs=(P("prow", "pcol"), P()), check_vma=False
    )
```

```python
import jax
import jax.numpy as jnp
from jax import lax
from jax.experimental import pallas as pl
from jax.experimental.pallas import tpu as pltpu
from jax.sharding import PartitionSpec as P


NB = 128
WIDE = 2 * NB
STRIP = 8
LEVELS, CORES = 8, 2

f32, bf16 = jnp.float32, jnp.bfloat16


def three_parts(value):
    first = value.astype(bf16).astype(f32)
    rest = value - first
    second = rest.astype(bf16).astype(f32)
    return first, second, (rest - second).astype(bf16).astype(f32)


def strip_product(left, right):
    a, b, c = three_parts(left)
    d, e, f = three_parts(right)
    return lax.dot_general(
        jnp.concatenate([a, a, b, b, a, c], axis=0).astype(bf16),
        jnp.concatenate([d, e, d, e, f, d], axis=0).astype(bf16),
        (((0,), (0,)), ((), ())),
        preferred_element_type=f32,
    )


def strip_columns(rows, first, lanes):
    return [
        jnp.sum(jnp.where(lanes == first + c, rows, 0.0), axis=1, keepdims=True)
        for c in range(STRIP)
    ]


def identity_matrix():
    rows = lax.broadcasted_iota(jnp.int32, (WIDE, WIDE), 0)
    return (rows == lax.broadcasted_iota(jnp.int32, (WIDE, WIDE), 1)).astype(f32)


def strips_of(half):
    count = WIDE // STRIP // 2
    return half * count, (half + 1) * count


def cholesky_kernel(gram_ref, upper_ref, inverse_ref, work):
    work[:, :WIDE] = gram_ref[...]
    work[:, WIDE:] = identity_matrix()
    lanes = lax.broadcasted_iota(jnp.int32, (STRIP, WIDE), 1)
    row_ids = lax.broadcasted_iota(jnp.int32, (STRIP, WIDE), 0)
    sub_narrow = lax.broadcasted_iota(jnp.int32, (STRIP, 1), 0)
    sub_wide = lax.broadcasted_iota(jnp.int32, (STRIP, 2 * WIDE), 0)
    for half in range(2):
        low, high = half * NB, half * NB + 3 * NB

        def strip(index, carry):
            first = pl.multiple_of(index * STRIP, STRIP)
            rows = work[pl.ds(first, STRIP), :]
            diag = strip_columns(rows[:, :WIDE], first, lanes)
            for c in range(STRIP):
                inverse = lax.rsqrt(diag[c][c : c + 1])
                pivot_row = rows[c : c + 1] * inverse
                factor = jnp.where(sub_narrow > c, diag[c] * inverse, 0.0)
                for d in range(c + 1, STRIP):
                    diag[d] = diag[d] - factor * (diag[d][c : c + 1] * inverse)
                rows = jnp.where(sub_wide == c, pivot_row, rows - factor * pivot_row)
            upper_ref[pl.ds(first, STRIP), :] = jnp.where(
                lanes >= first + row_ids, rows[:, :WIDE], 0.0
            )
            inverse_ref[pl.ds(first, STRIP), :] = rows[:, WIDE:]
            left = jnp.where(lanes >= first + STRIP, rows[:, :WIDE], 0.0)[:, low:]
            work[low:, low:high] = work[low:, low:high] - strip_product(left, rows[:, low:high])
            return carry

        lax.fori_loop(*strips_of(half), strip, 0)


def lower_upper_kernel(
    square_ref, turned_ref, upper_ref, unit_ref, unit_inv_ref, upper_inv_ref, work, turned_work
):
    work[:, :WIDE] = square_ref[...]
    work[:, WIDE:] = identity_matrix()
    turned_work[:, :WIDE] = turned_ref[...]
    turned_work[:, WIDE:] = identity_matrix()
    lanes = lax.broadcasted_iota(jnp.int32, (STRIP, WIDE), 1)
    row_ids = lax.broadcasted_iota(jnp.int32, (STRIP, WIDE), 0)
    sub_narrow = lax.broadcasted_iota(jnp.int32, (STRIP, 1), 0)
    sub_wide = lax.broadcasted_iota(jnp.int32, (STRIP, 2 * WIDE), 0)
    for half in range(2):
        low, high = half * NB, half * NB + 3 * NB

        def strip(index, carry):
            first = pl.multiple_of(index * STRIP, STRIP)
            rows = work[pl.ds(first, STRIP), :]
            turned = turned_work[pl.ds(first, STRIP), :]
            diag = strip_columns(rows[:, :WIDE], first, lanes)
            diag_turned = strip_columns(turned[:, :WIDE], first, lanes)
            for c in range(STRIP):
                inverse = 1.0 / diag[c][c : c + 1]
                factor = jnp.where(sub_narrow > c, diag[c] * inverse, 0.0)
                factor_turned = jnp.where(sub_narrow > c, diag_turned[c], 0.0)
                for d in range(c + 1, STRIP):
                    diag[d] = diag[d] - factor * diag[d][c : c + 1]
                    diag_turned[d] = diag_turned[d] - factor_turned * (
                        diag_turned[d][c : c + 1] * inverse
                    )
                rows = rows - factor * rows[c : c + 1]
                pivot_row = turned[c : c + 1] * inverse
                turned = jnp.where(sub_wide == c, pivot_row, turned - factor_turned * pivot_row)
            kept = lanes >= first + row_ids
            upper_ref[pl.ds(first, STRIP), :] = jnp.where(kept, rows[:, :WIDE], 0.0)
            unit_ref[pl.ds(first, STRIP), :] = jnp.where(kept, turned[:, :WIDE], 0.0)
            unit_inv_ref[pl.ds(first, STRIP), :] = rows[:, WIDE:]
            upper_inv_ref[pl.ds(first, STRIP), :] = turned[:, WIDE:]
            after = lanes >= first + STRIP
            left = jnp.where(after, rows[:, :WIDE], 0.0)[:, low:]
            left_turned = jnp.where(after, turned[:, :WIDE], 0.0)[:, low:]
            work[low:, low:high] = work[low:, low:high] - strip_product(
                left_turned, rows[:, low:high]
            )
            turned_work[low:, low:high] = turned_work[low:, low:high] - strip_product(
                left, turned[:, low:high]
            )
            return carry

        lax.fori_loop(*strips_of(half), strip, 0)


square_shape = jax.ShapeDtypeStruct((WIDE, WIDE), f32)


def cholesky(gram):
    return pl.pallas_call(
        cholesky_kernel,
        out_shape=(square_shape,) * 2,
        scratch_shapes=[pltpu.VMEM((WIDE, 2 * WIDE), f32)],
        cost_estimate=pl.CostEstimate(
            flops=14_000_000_000, bytes_accessed=800_000, transcendentals=0
        ),
        name="cholesky",
    )(gram)


def lower_upper(square):
    return pl.pallas_call(
        lower_upper_kernel,
        out_shape=(square_shape,) * 4,
        scratch_shapes=[pltpu.VMEM((WIDE, 2 * WIDE), f32)] * 2,
        cost_estimate=pl.CostEstimate(
            flops=15_000_000_000, bytes_accessed=1_600_000, transcendentals=0
        ),
        name="lower_upper",
    )(square, square.T)


def product(left, right, precision=lax.Precision.HIGHEST):
    return jnp.dot(left, right, precision=precision, preferred_element_type=f32)


def transposed_product(left, right, precision=lax.Precision.HIGHEST):
    return lax.dot_general(
        left, right, (((0,), (0,)), ((), ())), precision=precision, preferred_element_type=f32
    )


def update_kernel(
    flags, matrix_ref, shifted_ref, turned_ref, own_ref, sibling_ref, upper_ref, upper_inv_ref, out_ref, parts
):
    step = pl.program_id(0)

    def two_parts(value):
        first = value.astype(bf16)
        return first, (value - first.astype(f32)).astype(bf16)

    @pl.when(step == 0)
    def _():
        first, second = two_parts(shifted_ref[...])
        parts[:, :WIDE] = first
        parts[:, WIDE : 2 * WIDE] = first
        parts[:, 2 * WIDE :] = second

    core, packs, on_top = flags[0], (flags[1] == 1) & (step == 0), flags[2] == 1
    blocks = pl.num_programs(0) // CORES
    summed = jnp.where(core == step // blocks, own_ref[...], sibling_ref[...])
    a, b = two_parts(summed)
    c, d = two_parts(turned_ref[...])
    weights = jnp.dot(
        jnp.concatenate([a, a, b], axis=1),
        jnp.concatenate([c, d, c], axis=0),
        preferred_element_type=f32,
    )
    weights = jnp.where(packs, -upper_inv_ref[...], weights)
    first, second = two_parts(weights)
    update = lax.dot_general(
        parts[...],
        jnp.concatenate([first, second, first], axis=1),
        (((1,), (1,)), ((), ())),
        preferred_element_type=f32,
    )
    out_ref[...] = jnp.where(packs, 0.0, matrix_ref[...]) - update

    @pl.when(packs & on_top)
    def _():
        above = lax.broadcasted_iota(jnp.int32, (WIDE, WIDE), 0) <= lax.broadcasted_iota(
            jnp.int32, (WIDE, WIDE), 1
        )
        out_ref[:WIDE, :] = jnp.where(above, -upper_ref[...], out_ref[:WIDE, :])


def updated(flags, matrix, shifted, turned, own, sibling, upper, upper_inv):
    rows, cols = matrix.shape
    blocks = cols // WIDE
    whole = lambda shape: pl.BlockSpec(shape, lambda n, flags: (0, 0))
    columns = pl.BlockSpec((rows, WIDE), lambda n, flags: (0, n))
    half = pl.BlockSpec((WIDE, WIDE), lambda n, flags: (n % (blocks // CORES), 0))
    square = whole((WIDE, WIDE))
    return pl.pallas_call(
        update_kernel,
        grid_spec=pltpu.PrefetchScalarGridSpec(
            num_scalar_prefetch=1,
            grid=(blocks,),
            in_specs=[columns, whole((rows, WIDE)), square, half, half, square, square],
            out_specs=columns,
            scratch_shapes=[pltpu.VMEM((rows, 3 * WIDE), bf16)],
        ),
        out_shape=jax.ShapeDtypeStruct(matrix.shape, f32),
        cost_estimate=pl.CostEstimate(
            flops=5_000_000_000, bytes_accessed=16_000_000, transcendentals=0
        ),
        name="update",
    )(flags, matrix, shifted, turned, own, sibling, upper, upper_inv)


def exchange(pieces, axis, groups=None):
    return lax.all_to_all(pieces, axis, 0, 0, axis_index_groups=groups)


def gather(piece, axis, count, groups=None):
    return exchange(jnp.broadcast_to(piece, (count, *piece.shape)), axis, groups)


def per_device(matrix):
    my_row, my_col = lax.axis_index("prow"), lax.axis_index("pcol")
    rows_count, cols_count = lax.axis_size("prow"), lax.axis_size("pcol")
    core, level = my_row % CORES, my_row // CORES
    on_top, has_panel = my_row == 0, my_col == 0
    levels = [[CORES * z + c for z in range(LEVELS)] for c in range(CORES)]
    rows, _ = matrix.shape
    high = lax.Precision.HIGH

    def permute(value, pairs):
        return lax.ppermute(value, "prow", pairs)

    def swap(value):
        return permute(value, [(i, i ^ 1) for i in range(rows_count)])

    def halves(value):
        low, high = value[: value.shape[0] // CORES], value[value.shape[0] // CORES :]
        return jnp.where(core == 0, low, high), jnp.where(core == 0, high, low)

    panel = matrix[:, :WIDE]
    panel_piece = exchange(panel.reshape(cols_count, -1, WIDE), "pcol")[0]

    low, high_half = jnp.split(matrix[:WIDE].T, CORES)
    top_half = jnp.where(core == 0, low, permute(high_half, [(0, 1)]))
    top_half = top_half.reshape(LEVELS, -1, WIDE)
    top_slice = jnp.where(level == 0, top_half[0], 0.0)
    for z in range(1, LEVELS):
        top_slice = top_slice + permute(
            top_half[z], [(c, CORES * z + c) for c in range(CORES)]
        )
    panel_piece, top_slice = lax.optimization_barrier((panel_piece, top_slice))
    panel = gather(panel_piece, "pcol", cols_count).reshape(rows, WIDE)

    own_top = jnp.where(on_top, panel[:WIDE], 0.0)
    squares = [transposed_product(panel, panel), own_top]
    squares = jnp.concatenate([a.reshape(rows_count, -1, WIDE) for a in squares], axis=1)
    square_piece = exchange(squares, "prow").sum(0)

    mine, other = halves(transposed_product(matrix, panel, high))
    mine = mine + swap(other)
    square_piece, mine = lax.optimization_barrier((square_piece, mine))
    summed = exchange(mine.reshape(LEVELS, -1, WIDE), "prow", levels)
    squares = lax.all_gather(square_piece, "prow")
    gram, top = (a.reshape(WIDE, WIDE) for a in jnp.split(squares, 2, axis=1))
    upper, inverse = cholesky(gram)
    summed = summed.sum(0) + product(top_slice, upper)
    summed = gather(summed, "prow", LEVELS, levels).reshape(-1, WIDE)
    sibling = swap(summed)

    wy_upper, _, unit_inv, upper_inv = lower_upper(top + upper)
    turned = transposed_product(inverse, transposed_product(unit_inv, upper_inv))
    shifted = jnp.concatenate(
        [jnp.where(on_top, panel[:WIDE] + upper, panel[:WIDE]), panel[WIDE:]], axis=0
    )
    flags = jnp.stack([core, has_panel.astype(jnp.int32), on_top.astype(jnp.int32)])
    result = updated(flags, matrix, shifted, turned, summed, sibling, upper, upper_inv)
    factors = [
        product(wy_upper[s, s], product(inverse[s, s].T, unit_inv[s, s].T))
        for s in (slice(0, NB), slice(NB, WIDE))
    ]
    return (result, jnp.stack(factors))


def solution(mesh):
    placed = (P("prow", "pcol"),)
    return jax.shard_map(
        per_device, mesh=mesh, in_specs=placed, out_specs=(P("prow", "pcol"), P()), check_vma=False
    )
```

```python
import jax
import jax.numpy as jnp
from jax import lax
from jax.experimental import pallas as pl
from jax.experimental.pallas import tpu as pltpu
from jax.sharding import PartitionSpec as P


NB = 128
WIDE = 2 * NB
STRIP = 8
LEVELS, CORES = 8, 2

f32, bf16 = jnp.float32, jnp.bfloat16


def three_parts(value):
    first = value.astype(bf16).astype(f32)
    rest = value - first
    second = rest.astype(bf16).astype(f32)
    return first, second, (rest - second).astype(bf16).astype(f32)


def strip_product(left, right):
    a, b, c = three_parts(left)
    d, e, f = three_parts(right)
    return lax.dot_general(
        jnp.concatenate([a, a, b, b, a, c], axis=0).astype(bf16),
        jnp.concatenate([d, e, d, e, f, d], axis=0).astype(bf16),
        (((0,), (0,)), ((), ())),
        preferred_element_type=f32,
    )


def strip_columns(rows, first, lanes):
    return [
        jnp.sum(jnp.where(lanes == first + c, rows, 0.0), axis=1, keepdims=True)
        for c in range(STRIP)
    ]


def identity_matrix():
    rows = lax.broadcasted_iota(jnp.int32, (WIDE, WIDE), 0)
    return (rows == lax.broadcasted_iota(jnp.int32, (WIDE, WIDE), 1)).astype(f32)


def strips_of(half):
    count = WIDE // STRIP // 2
    return half * count, (half + 1) * count


def cholesky_kernel(gram_ref, upper_ref, inverse_ref, work):
    work[:, :WIDE] = gram_ref[...]
    work[:, WIDE:] = identity_matrix()
    lanes = lax.broadcasted_iota(jnp.int32, (STRIP, WIDE), 1)
    row_ids = lax.broadcasted_iota(jnp.int32, (STRIP, WIDE), 0)
    sub_narrow = lax.broadcasted_iota(jnp.int32, (STRIP, 1), 0)
    sub_wide = lax.broadcasted_iota(jnp.int32, (STRIP, 2 * WIDE), 0)
    for half in range(2):
        low, high = half * NB, half * NB + 3 * NB

        def strip(index, carry):
            first = pl.multiple_of(index * STRIP, STRIP)
            rows = work[pl.ds(first, STRIP), :]
            diag = strip_columns(rows[:, :WIDE], first, lanes)
            for c in range(STRIP):
                inverse = lax.rsqrt(diag[c][c : c + 1])
                pivot_row = rows[c : c + 1] * inverse
                factor = jnp.where(sub_narrow > c, diag[c] * inverse, 0.0)
                for d in range(c + 1, STRIP):
                    diag[d] = diag[d] - factor * (diag[d][c : c + 1] * inverse)
                rows = jnp.where(sub_wide == c, pivot_row, rows - factor * pivot_row)
            upper_ref[pl.ds(first, STRIP), :] = jnp.where(
                lanes >= first + row_ids, rows[:, :WIDE], 0.0
            )
            inverse_ref[pl.ds(first, STRIP), :] = rows[:, WIDE:]
            left = jnp.where(lanes >= first + STRIP, rows[:, :WIDE], 0.0)[:, low:]
            work[low:, low:high] = work[low:, low:high] - strip_product(left, rows[:, low:high])
            return carry

        lax.fori_loop(*strips_of(half), strip, 0)


def sharp_product(left, right, right_turned=False):
    a, b, c = three_parts(left)
    d, e, f = three_parts(right)
    axis = 1 if right_turned else 0
    return lax.dot_general(
        jnp.concatenate([a, a, b, b, a, c], axis=1).astype(bf16),
        jnp.concatenate([d, e, d, e, f, d], axis=axis).astype(bf16),
        (((1,), (axis,)), ((), ())),
        preferred_element_type=f32,
    )


def lower_upper_kernel(
    top_ref, r_ref, inverse_ref, square_ref, factors_ref, panel_ref, work, turned_work
):
    total = top_ref[...] + r_ref[...]
    work[:, :WIDE] = total
    work[:, WIDE:] = identity_matrix()
    turned_work[:, :WIDE] = total.T
    turned_work[:, WIDE:] = identity_matrix()
    lanes = lax.broadcasted_iota(jnp.int32, (STRIP, WIDE), 1)
    row_ids = lax.broadcasted_iota(jnp.int32, (STRIP, WIDE), 0)
    sub_narrow = lax.broadcasted_iota(jnp.int32, (STRIP, 1), 0)
    sub_wide = lax.broadcasted_iota(jnp.int32, (STRIP, 2 * WIDE), 0)
    for half in range(2):
        low, high = half * NB, half * NB + 3 * NB

        def strip(index, carry):
            first = pl.multiple_of(index * STRIP, STRIP)
            rows = work[pl.ds(first, STRIP), :]
            turned = turned_work[pl.ds(first, STRIP), :]
            diag = strip_columns(rows[:, :WIDE], first, lanes)
            diag_turned = strip_columns(turned[:, :WIDE], first, lanes)
            for c in range(STRIP):
                inverse = 1.0 / diag[c][c : c + 1]
                factor = jnp.where(sub_narrow > c, diag[c] * inverse, 0.0)
                factor_turned = jnp.where(sub_narrow > c, diag_turned[c], 0.0)
                for d in range(c + 1, STRIP):
                    diag[d] = diag[d] - factor * diag[d][c : c + 1]
                    diag_turned[d] = diag_turned[d] - factor_turned * (
                        diag_turned[d][c : c + 1] * inverse
                    )
                rows = rows - factor * rows[c : c + 1]
                pivot_row = turned[c : c + 1] * inverse
                turned = jnp.where(sub_wide == c, pivot_row, turned - factor_turned * pivot_row)
            after = lanes >= first + STRIP
            left = jnp.where(after, rows[:, :WIDE], 0.0)[:, low:]
            left_turned = jnp.where(after, turned[:, :WIDE], 0.0)[:, low:]
            work[low:, low:high] = work[low:, low:high] - strip_product(
                left_turned, rows[:, low:high]
            )
            turned_work[low:, low:high] = turned_work[low:, low:high] - strip_product(
                left, turned[:, low:high]
            )
            kept = lanes >= first + row_ids
            work[pl.ds(first, STRIP), :WIDE] = jnp.where(kept, rows[:, :WIDE], 0.0)
            work[pl.ds(first, STRIP), WIDE:] = rows[:, WIDE:]
            turned_work[pl.ds(first, STRIP), WIDE:] = turned[:, WIDE:]
            return carry

        lax.fori_loop(*strips_of(half), strip, 0)
    inner = sharp_product(work[:, WIDE:], inverse_ref[...])
    upper_inv = turned_work[:, WIDE:].T
    square_ref[...] = sharp_product(upper_inv, inner)
    panel_ref[...] = -upper_inv
    for k in range(2):
        block = slice(k * NB, (k + 1) * NB)
        factors_ref[k] = sharp_product(work[block, block], inner[block, block], right_turned=True)


square_shape = jax.ShapeDtypeStruct((WIDE, WIDE), f32)


def cholesky(gram):
    return pl.pallas_call(
        cholesky_kernel,
        out_shape=(square_shape,) * 2,
        scratch_shapes=[pltpu.VMEM((WIDE, 2 * WIDE), f32)],
        cost_estimate=pl.CostEstimate(
            flops=14_000_000_000, bytes_accessed=800_000, transcendentals=0
        ),
        name="cholesky",
    )(gram)


def lower_upper(top, r, inverse):
    return pl.pallas_call(
        lower_upper_kernel,
        out_shape=(square_shape, jax.ShapeDtypeStruct((2, NB, NB), f32), square_shape),
        scratch_shapes=[pltpu.VMEM((WIDE, 2 * WIDE), f32)] * 2,
        cost_estimate=pl.CostEstimate(
            flops=17_000_000_000, bytes_accessed=1_600_000, transcendentals=0
        ),
        name="lower_upper",
    )(top, r, inverse)


def product(left, right, precision=lax.Precision.HIGHEST):
    return jnp.dot(left, right, precision=precision, preferred_element_type=f32)


def transposed_product(left, right, precision=lax.Precision.HIGHEST):
    return lax.dot_general(
        left, right, (((0,), (0,)), ((), ())), precision=precision, preferred_element_type=f32
    )


def exchange(pieces, axis, groups=None):
    return lax.all_to_all(pieces, axis, 0, 0, axis_index_groups=groups)


def gather(piece, axis, count, groups=None):
    return exchange(jnp.broadcast_to(piece, (count, *piece.shape)), axis, groups)


def per_device(matrix):
    my_row, my_col = lax.axis_index("prow"), lax.axis_index("pcol")
    rows_count, cols_count = lax.axis_size("prow"), lax.axis_size("pcol")
    core, level = my_row % CORES, my_row // CORES
    on_top, has_panel = my_row == 0, my_col == 0
    levels = [[CORES * z + c for z in range(LEVELS)] for c in range(CORES)]
    rows, cols = matrix.shape
    high = lax.Precision.HIGH

    def permute(value, pairs):
        return lax.ppermute(value, "prow", pairs)

    def swap(value):
        return permute(value, [(i, i ^ 1) for i in range(rows_count)])

    def halves(value):
        low, high = value[: value.shape[0] // CORES], value[value.shape[0] // CORES :]
        return jnp.where(core == 0, low, high), jnp.where(core == 0, high, low)

    column_ids = lax.broadcasted_iota(jnp.int32, (1, cols), 1)
    replaced = has_panel & (column_ids < WIDE)
    pieces, top_rows, source = lax.optimization_barrier(
        (matrix[:, :WIDE].reshape(cols_count, -1, WIDE), matrix[:WIDE], matrix)
    )
    panel_piece = exchange(pieces, "pcol")[0]
    base = jnp.where(replaced, 0.0, source)
    low, high_half = jnp.split(top_rows.T, CORES)
    panel_piece, base = lax.optimization_barrier((panel_piece, base))
    panel = gather(panel_piece, "pcol", cols_count).reshape(rows, WIDE)

    top_half = jnp.where(core == 0, low, permute(high_half, [(0, 1)]))
    held = top_half.reshape(LEVELS, -1, WIDE)
    step = LEVELS // 2
    while step:
        givers = range(0, LEVELS, 2 * step)
        pairs = [(CORES * z + c, CORES * (z + step) + c) for z in givers for c in range(CORES)]
        received = permute(held[step:], pairs)
        held = jnp.where(level % (2 * step) == 0, held[:step], received)
        step //= 2
    panel, top_slice = lax.optimization_barrier((panel, held[0]))

    own_top = jnp.where(on_top, panel[:WIDE], 0.0)
    squares = [transposed_product(panel, panel), own_top]
    squares = jnp.concatenate([a.reshape(rows_count, -1, WIDE) for a in squares], axis=1)
    squares, panel = lax.optimization_barrier((squares, panel))
    square_piece = exchange(squares, "prow")
    mine, other = halves(transposed_product(base, panel, high))
    square_piece = square_piece.sum(0)
    mine = mine + swap(other)
    squares, mine = lax.optimization_barrier((lax.all_gather(square_piece, "prow"), mine))
    gram, top = (a.reshape(WIDE, WIDE) for a in jnp.split(squares, 2, axis=1))
    summed = exchange(mine.reshape(LEVELS, -1, WIDE), "prow", levels).sum(0)
    upper, inverse = cholesky(gram)
    summed = summed + product(top_slice, upper)
    summed = gather(summed, "prow", LEVELS, levels).reshape(-1, WIDE)
    square, factors, panel_weights = lower_upper(top, upper, inverse)
    shifted = jnp.concatenate(
        [jnp.where(on_top, panel[:WIDE] + upper, panel[:WIDE]), panel[WIDE:]], axis=0
    )
    above = jnp.triu(jnp.ones((WIDE, WIDE), jnp.bool_))
    corner = jnp.where(above, -upper - jnp.eye(WIDE, dtype=f32), 0.0)
    corner = jnp.where(on_top & has_panel, corner, base[:WIDE, :WIDE])
    base = base.at[:WIDE, :WIDE].set(corner)
    sibling = swap(summed)
    mine, other = (
        lax.dot_general(
            square, a, (((1,), (1,)), ((), ())), precision=high, preferred_element_type=f32
        )
        for a in (summed, sibling)
    )
    weights = jnp.where(
        core == 0,
        jnp.concatenate([mine, other], axis=1),
        jnp.concatenate([other, mine], axis=1),
    )
    weights = weights.at[:, :WIDE].set(jnp.where(has_panel, panel_weights, weights[:, :WIDE]))
    return (base - product(shifted, weights, high), factors)


def solution(mesh):
    placed = (P("prow", "pcol"),)
    return jax.shard_map(
        per_device, mesh=mesh, in_specs=placed, out_specs=(P("prow", "pcol"), P()), check_vma=False
    )
```

```python
import jax
import jax.numpy as jnp
from jax import lax
from jax.experimental import pallas as pl
from jax.experimental.pallas import tpu as pltpu
from jax.experimental.layout import Layout, with_layout_constraint
from jax.sharding import PartitionSpec as P


NB = 128
WIDE = 2 * NB
STRIP = 8
LEVELS, CORES = 8, 2

f32, bf16 = jnp.float32, jnp.bfloat16


def three_parts(value):
    first = value.astype(bf16).astype(f32)
    rest = value - first
    second = rest.astype(bf16).astype(f32)
    return first, second, (rest - second).astype(bf16).astype(f32)


def strip_product(left, right):
    a, b, c = three_parts(left)
    d, e, f = three_parts(right)
    return lax.dot_general(
        jnp.concatenate([a, a, b, b, a, c], axis=0).astype(bf16),
        jnp.concatenate([d, e, d, e, f, d], axis=0).astype(bf16),
        (((0,), (0,)), ((), ())),
        preferred_element_type=f32,
    )


def strip_columns(rows, first, lanes):
    return [
        jnp.sum(jnp.where(lanes == first + c, rows, 0.0), axis=1, keepdims=True)
        for c in range(STRIP)
    ]


def identity_matrix():
    rows = lax.broadcasted_iota(jnp.int32, (WIDE, WIDE), 0)
    return (rows == lax.broadcasted_iota(jnp.int32, (WIDE, WIDE), 1)).astype(f32)


def strips_of(half):
    count = WIDE // STRIP // 2
    return half * count, (half + 1) * count


def cholesky_kernel(gram_ref, upper_ref, inverse_ref, work):
    work[:, :WIDE] = gram_ref[...]
    work[:, WIDE:] = identity_matrix()
    lanes = lax.broadcasted_iota(jnp.int32, (STRIP, WIDE), 1)
    row_ids = lax.broadcasted_iota(jnp.int32, (STRIP, WIDE), 0)
    sub_narrow = lax.broadcasted_iota(jnp.int32, (STRIP, 1), 0)
    sub_wide = lax.broadcasted_iota(jnp.int32, (STRIP, 2 * WIDE), 0)
    for half in range(2):
        low, high = half * NB, half * NB + 3 * NB

        def strip(index, carry):
            first = pl.multiple_of(index * STRIP, STRIP)
            rows = work[pl.ds(first, STRIP), :]
            diag = strip_columns(rows[:, :WIDE], first, lanes)
            for c in range(STRIP):
                inverse = lax.rsqrt(diag[c][c : c + 1])
                pivot_row = rows[c : c + 1] * inverse
                factor = jnp.where(sub_narrow > c, diag[c] * inverse, 0.0)
                for d in range(c + 1, STRIP):
                    diag[d] = diag[d] - factor * (diag[d][c : c + 1] * inverse)
                rows = jnp.where(sub_wide == c, pivot_row, rows - factor * pivot_row)
            upper_ref[pl.ds(first, STRIP), :] = jnp.where(
                lanes >= first + row_ids, rows[:, :WIDE], 0.0
            )
            inverse_ref[pl.ds(first, STRIP), :] = rows[:, WIDE:]
            left = jnp.where(lanes >= first + STRIP, rows[:, :WIDE], 0.0)[:, low:]
            work[low:, low:high] = work[low:, low:high] - strip_product(left, rows[:, low:high])
            return carry

        lax.fori_loop(*strips_of(half), strip, 0)


def sharp_product(left, right, right_turned=False):
    a, b, c = three_parts(left)
    d, e, f = three_parts(right)
    axis = 1 if right_turned else 0
    return lax.dot_general(
        jnp.concatenate([a, a, b, b, a, c], axis=1).astype(bf16),
        jnp.concatenate([d, e, d, e, f, d], axis=axis).astype(bf16),
        (((1,), (axis,)), ((), ())),
        preferred_element_type=f32,
    )


def lower_upper_kernel(
    top_ref, r_ref, inverse_ref, square_ref, factors_ref, panel_ref, work, turned_work
):
    total = top_ref[...] + r_ref[...]
    work[:, :WIDE] = total
    work[:, WIDE:] = identity_matrix()
    turned_work[:, :WIDE] = total.T
    turned_work[:, WIDE:] = identity_matrix()
    lanes = lax.broadcasted_iota(jnp.int32, (STRIP, WIDE), 1)
    row_ids = lax.broadcasted_iota(jnp.int32, (STRIP, WIDE), 0)
    sub_narrow = lax.broadcasted_iota(jnp.int32, (STRIP, 1), 0)
    sub_wide = lax.broadcasted_iota(jnp.int32, (STRIP, 2 * WIDE), 0)
    for half in range(2):
        low, high = half * NB, half * NB + 3 * NB

        def strip(index, carry):
            first = pl.multiple_of(index * STRIP, STRIP)
            rows = work[pl.ds(first, STRIP), :]
            turned = turned_work[pl.ds(first, STRIP), :]
            diag = strip_columns(rows[:, :WIDE], first, lanes)
            diag_turned = strip_columns(turned[:, :WIDE], first, lanes)
            for c in range(STRIP):
                inverse = 1.0 / diag[c][c : c + 1]
                factor = jnp.where(sub_narrow > c, diag[c] * inverse, 0.0)
                factor_turned = jnp.where(sub_narrow > c, diag_turned[c], 0.0)
                for d in range(c + 1, STRIP):
                    diag[d] = diag[d] - factor * diag[d][c : c + 1]
                    diag_turned[d] = diag_turned[d] - factor_turned * (
                        diag_turned[d][c : c + 1] * inverse
                    )
                rows = rows - factor * rows[c : c + 1]
                pivot_row = turned[c : c + 1] * inverse
                turned = jnp.where(sub_wide == c, pivot_row, turned - factor_turned * pivot_row)
            after = lanes >= first + STRIP
            left = jnp.where(after, rows[:, :WIDE], 0.0)[:, low:]
            left_turned = jnp.where(after, turned[:, :WIDE], 0.0)[:, low:]
            work[low:, low:high] = work[low:, low:high] - strip_product(
                left_turned, rows[:, low:high]
            )
            turned_work[low:, low:high] = turned_work[low:, low:high] - strip_product(
                left, turned[:, low:high]
            )
            kept = lanes >= first + row_ids
            work[pl.ds(first, STRIP), :WIDE] = jnp.where(kept, rows[:, :WIDE], 0.0)
            work[pl.ds(first, STRIP), WIDE:] = rows[:, WIDE:]
            turned_work[pl.ds(first, STRIP), WIDE:] = turned[:, WIDE:]
            return carry

        lax.fori_loop(*strips_of(half), strip, 0)
    inner = sharp_product(work[:, WIDE:], inverse_ref[...])
    upper_inv = turned_work[:, WIDE:].T
    square_ref[...] = sharp_product(upper_inv, inner)
    panel_ref[...] = -upper_inv
    for k in range(2):
        block = slice(k * NB, (k + 1) * NB)
        factors_ref[k] = sharp_product(work[block, block], inner[block, block], right_turned=True)


square_shape = jax.ShapeDtypeStruct((WIDE, WIDE), f32)


def cholesky(gram):
    return pl.pallas_call(
        cholesky_kernel,
        out_shape=(square_shape,) * 2,
        scratch_shapes=[pltpu.VMEM((WIDE, 2 * WIDE), f32)],
        cost_estimate=pl.CostEstimate(
            flops=14_000_000_000, bytes_accessed=800_000, transcendentals=0
        ),
        name="cholesky",
    )(gram)


def lower_upper(top, r, inverse):
    return pl.pallas_call(
        lower_upper_kernel,
        out_shape=(square_shape, jax.ShapeDtypeStruct((2, NB, NB), f32), square_shape),
        scratch_shapes=[pltpu.VMEM((WIDE, 2 * WIDE), f32)] * 2,
        cost_estimate=pl.CostEstimate(
            flops=17_000_000_000, bytes_accessed=1_600_000, transcendentals=0
        ),
        name="lower_upper",
    )(top, r, inverse)


def product(left, right, precision=lax.Precision.HIGHEST):
    return jnp.dot(left, right, precision=precision, preferred_element_type=f32)


def transposed_product(left, right, precision=lax.Precision.HIGHEST):
    return lax.dot_general(
        left, right, (((0,), (0,)), ((), ())), precision=precision, preferred_element_type=f32
    )


def exchange(pieces, axis, groups=None):
    return lax.all_to_all(pieces, axis, 0, 0, axis_index_groups=groups)


def gather(piece, axis, count, groups=None):
    return exchange(jnp.broadcast_to(piece, (count, *piece.shape)), axis, groups)


def per_device(matrix):
    my_row, my_col = lax.axis_index("prow"), lax.axis_index("pcol")
    rows_count, cols_count = lax.axis_size("prow"), lax.axis_size("pcol")
    core, level = my_row % CORES, my_row // CORES
    on_top, has_panel = my_row == 0, my_col == 0
    levels = [[CORES * z + c for z in range(LEVELS)] for c in range(CORES)]
    rows, cols = matrix.shape
    high = lax.Precision.HIGH

    def permute(value, pairs):
        return lax.ppermute(value, "prow", pairs)

    def swap(value):
        return permute(value, [(i, i ^ 1) for i in range(rows_count)])

    def halves(value):
        low, high = value[: value.shape[0] // CORES], value[value.shape[0] // CORES :]
        return jnp.where(core == 0, low, high), jnp.where(core == 0, high, low)

    column_ids = lax.broadcasted_iota(jnp.int32, (1, cols), 1)
    replaced = has_panel & (column_ids < WIDE)
    pieces = matrix[:, :WIDE].reshape(cols_count, -1, WIDE)
    panel_piece = exchange(pieces, "pcol")[0]
    low, high_half = jnp.split(matrix[:WIDE].T, CORES)
    panel = gather(panel_piece, "pcol", cols_count).reshape(rows, WIDE)

    top_half = jnp.where(core == 0, low, permute(high_half, [(0, 1)]))
    held = top_half.reshape(LEVELS, -1, WIDE)
    step = LEVELS // 2
    while step:
        givers = range(0, LEVELS, 2 * step)
        pairs = [(CORES * z + c, CORES * (z + step) + c) for z in givers for c in range(CORES)]
        received = permute(held[step:], pairs)
        held = jnp.where(level % (2 * step) == 0, held[:step], received)
        step //= 2
    panel, top_slice = lax.optimization_barrier((panel, held[0]))

    strip = WIDE // cols_count
    squares = [
        lax.dynamic_slice_in_dim(a, my_col * strip, strip, 0)
        for a in (transposed_product(panel, panel), panel)
    ]
    squares = jnp.concatenate([squares[0], jnp.where(on_top, squares[1], 0.0)], axis=0)
    square_piece, panel = lax.optimization_barrier((lax.all_gather(squares, "prow"), panel))
    squares = gather(square_piece.sum(0), "pcol", cols_count)
    mine, other = halves(transposed_product(matrix, panel, high))
    mine = with_layout_constraint(mine + swap(other), Layout((0, 1)))
    squares, mine = lax.optimization_barrier((squares, mine))
    gram, top = (a.reshape(WIDE, WIDE) for a in jnp.split(squares, 2, axis=1))
    summed = exchange(mine.reshape(LEVELS, -1, WIDE), "prow", levels)
    base = lax.optimization_barrier(jnp.where(replaced, 0.0, matrix))
    summed = summed.sum(0)
    upper, inverse = cholesky(gram)
    summed = summed + product(top_slice, upper)
    summed = gather(summed, "prow", LEVELS, levels).reshape(-1, WIDE)
    square, factors, panel_weights = lower_upper(top, upper, inverse)
    shifted = jnp.concatenate(
        [jnp.where(on_top, panel[:WIDE] + upper, panel[:WIDE]), panel[WIDE:]], axis=0
    )
    above = jnp.triu(jnp.ones((WIDE, WIDE), jnp.bool_))
    corner = jnp.where(above, -upper - jnp.eye(WIDE, dtype=f32), 0.0)
    corner = jnp.where(on_top & has_panel, corner, base[:WIDE, :WIDE])
    base = base.at[:WIDE, :WIDE].set(corner)
    sibling = swap(summed)
    mine, other = (
        lax.dot_general(
            square, a, (((1,), (1,)), ((), ())), precision=high, preferred_element_type=f32
        )
        for a in (summed, sibling)
    )
    weights = jnp.where(
        core == 0,
        jnp.concatenate([mine, other], axis=1),
        jnp.concatenate([other, mine], axis=1),
    )
    weights = weights.at[:, :WIDE].set(jnp.where(has_panel, panel_weights, weights[:, :WIDE]))
    return (base - product(shifted, weights, high), factors)


def solution(mesh):
    placed = (P("prow", "pcol"),)
    return jax.shard_map(
        per_device, mesh=mesh, in_specs=placed, out_specs=(P("prow", "pcol"), P()), check_vma=False
    )
```

```python
import jax
import jax.numpy as jnp
from jax import lax
from jax.experimental import pallas as pl
from jax.experimental.pallas import tpu as pltpu
from jax.sharding import PartitionSpec as P


NB = 128
WIDE = 2 * NB
STRIP = 8
LEVELS, CORES = 8, 2

f32, bf16 = jnp.float32, jnp.bfloat16


def three_parts(value):
    first = value.astype(bf16).astype(f32)
    rest = value - first
    second = rest.astype(bf16).astype(f32)
    return first, second, (rest - second).astype(bf16).astype(f32)


def strip_product(left, right):
    a, b, c = three_parts(left)
    d, e, f = three_parts(right)
    return lax.dot_general(
        jnp.concatenate([a, a, b, b, a, c], axis=0).astype(bf16),
        jnp.concatenate([d, e, d, e, f, d], axis=0).astype(bf16),
        (((0,), (0,)), ((), ())),
        preferred_element_type=f32,
    )


def strip_columns(rows, first, lanes):
    return [
        jnp.sum(jnp.where(lanes == first + c, rows, 0.0), axis=1, keepdims=True)
        for c in range(STRIP)
    ]


def identity_matrix():
    rows = lax.broadcasted_iota(jnp.int32, (WIDE, WIDE), 0)
    return (rows == lax.broadcasted_iota(jnp.int32, (WIDE, WIDE), 1)).astype(f32)


def strips_of(half):
    count = WIDE // STRIP // 2
    return half * count, (half + 1) * count


def cholesky_kernel(gram_ref, upper_ref, inverse_ref, work):
    work[:, :WIDE] = gram_ref[...]
    work[:, WIDE:] = identity_matrix()
    lanes = lax.broadcasted_iota(jnp.int32, (STRIP, WIDE), 1)
    row_ids = lax.broadcasted_iota(jnp.int32, (STRIP, WIDE), 0)
    sub_narrow = lax.broadcasted_iota(jnp.int32, (STRIP, 1), 0)
    sub_wide = lax.broadcasted_iota(jnp.int32, (STRIP, 2 * WIDE), 0)
    for half in range(2):
        low, high = half * NB, half * NB + 3 * NB

        def strip(index, carry):
            first = pl.multiple_of(index * STRIP, STRIP)
            rows = work[pl.ds(first, STRIP), :]
            diag = strip_columns(rows[:, :WIDE], first, lanes)
            for c in range(STRIP):
                inverse = lax.rsqrt(diag[c][c : c + 1])
                pivot_row = rows[c : c + 1] * inverse
                factor = jnp.where(sub_narrow > c, diag[c] * inverse, 0.0)
                for d in range(c + 1, STRIP):
                    diag[d] = diag[d] - factor * (diag[d][c : c + 1] * inverse)
                rows = jnp.where(sub_wide == c, pivot_row, rows - factor * pivot_row)
            upper_ref[pl.ds(first, STRIP), :] = jnp.where(
                lanes >= first + row_ids, rows[:, :WIDE], 0.0
            )
            inverse_ref[pl.ds(first, STRIP), :] = rows[:, WIDE:]
            left = jnp.where(lanes >= first + STRIP, rows[:, :WIDE], 0.0)[:, low:]
            work[low:, low:high] = work[low:, low:high] - strip_product(left, rows[:, low:high])
            return carry

        lax.fori_loop(*strips_of(half), strip, 0)


def sharp_product(left, right, right_turned=False):
    a, b, c = three_parts(left)
    d, e, f = three_parts(right)
    axis = 1 if right_turned else 0
    return lax.dot_general(
        jnp.concatenate([a, a, b, b, a, c], axis=1).astype(bf16),
        jnp.concatenate([d, e, d, e, f, d], axis=axis).astype(bf16),
        (((1,), (axis,)), ((), ())),
        preferred_element_type=f32,
    )


def lower_upper_kernel(
    top_ref, r_ref, inverse_ref, square_ref, factors_ref, panel_ref, work, turned_work
):
    total = top_ref[...] + r_ref[...]
    work[:, :WIDE] = total
    work[:, WIDE:] = identity_matrix()
    turned_work[:, :WIDE] = total.T
    turned_work[:, WIDE:] = identity_matrix()
    lanes = lax.broadcasted_iota(jnp.int32, (STRIP, WIDE), 1)
    row_ids = lax.broadcasted_iota(jnp.int32, (STRIP, WIDE), 0)
    sub_narrow = lax.broadcasted_iota(jnp.int32, (STRIP, 1), 0)
    sub_wide = lax.broadcasted_iota(jnp.int32, (STRIP, 2 * WIDE), 0)
    for half in range(2):
        low, high = half * NB, half * NB + 3 * NB

        def strip(index, carry):
            first = pl.multiple_of(index * STRIP, STRIP)
            rows = work[pl.ds(first, STRIP), :]
            turned = turned_work[pl.ds(first, STRIP), :]
            diag = strip_columns(rows[:, :WIDE], first, lanes)
            diag_turned = strip_columns(turned[:, :WIDE], first, lanes)
            for c in range(STRIP):
                inverse = 1.0 / diag[c][c : c + 1]
                factor = jnp.where(sub_narrow > c, diag[c] * inverse, 0.0)
                factor_turned = jnp.where(sub_narrow > c, diag_turned[c], 0.0)
                for d in range(c + 1, STRIP):
                    diag[d] = diag[d] - factor * diag[d][c : c + 1]
                    diag_turned[d] = diag_turned[d] - factor_turned * (
                        diag_turned[d][c : c + 1] * inverse
                    )
                rows = rows - factor * rows[c : c + 1]
                pivot_row = turned[c : c + 1] * inverse
                turned = jnp.where(sub_wide == c, pivot_row, turned - factor_turned * pivot_row)
            after = lanes >= first + STRIP
            left = jnp.where(after, rows[:, :WIDE], 0.0)[:, low:]
            left_turned = jnp.where(after, turned[:, :WIDE], 0.0)[:, low:]
            work[low:, low:high] = work[low:, low:high] - strip_product(
                left_turned, rows[:, low:high]
            )
            turned_work[low:, low:high] = turned_work[low:, low:high] - strip_product(
                left, turned[:, low:high]
            )
            kept = lanes >= first + row_ids
            work[pl.ds(first, STRIP), :WIDE] = jnp.where(kept, rows[:, :WIDE], 0.0)
            work[pl.ds(first, STRIP), WIDE:] = rows[:, WIDE:]
            turned_work[pl.ds(first, STRIP), WIDE:] = turned[:, WIDE:]
            return carry

        lax.fori_loop(*strips_of(half), strip, 0)
    inner = sharp_product(work[:, WIDE:], inverse_ref[...])
    upper_inv = turned_work[:, WIDE:].T
    square_ref[...] = sharp_product(upper_inv, inner)
    panel_ref[...] = -upper_inv
    for k in range(2):
        block = slice(k * NB, (k + 1) * NB)
        factors_ref[k] = sharp_product(work[block, block], inner[block, block], right_turned=True)


square_shape = jax.ShapeDtypeStruct((WIDE, WIDE), f32)


def cholesky(gram):
    return pl.pallas_call(
        cholesky_kernel,
        out_shape=(square_shape,) * 2,
        scratch_shapes=[pltpu.VMEM((WIDE, 2 * WIDE), f32)],
        cost_estimate=pl.CostEstimate(
            flops=14_000_000_000, bytes_accessed=800_000, transcendentals=0
        ),
        name="cholesky",
    )(gram)


def lower_upper(top, r, inverse):
    return pl.pallas_call(
        lower_upper_kernel,
        out_shape=(square_shape, jax.ShapeDtypeStruct((2, NB, NB), f32), square_shape),
        scratch_shapes=[pltpu.VMEM((WIDE, 2 * WIDE), f32)] * 2,
        cost_estimate=pl.CostEstimate(
            flops=17_000_000_000, bytes_accessed=1_600_000, transcendentals=0
        ),
        name="lower_upper",
    )(top, r, inverse)


def product(left, right, precision=lax.Precision.HIGHEST):
    return jnp.dot(left, right, precision=precision, preferred_element_type=f32)


def transposed_product(left, right, precision=lax.Precision.HIGHEST):
    return lax.dot_general(
        left, right, (((0,), (0,)), ((), ())), precision=precision, preferred_element_type=f32
    )


def join_kernel(flags, products_ref, received_ref, joined_ref):
    width = received_ref.shape[1]
    half = jnp.where(flags[0] == 0, products_ref[:, :width], products_ref[:, width:])
    joined_ref[...] = (half + received_ref[...]).T


def joined(core, products, received):
    vmem = pl.BlockSpec(memory_space=pltpu.VMEM)
    return pl.pallas_call(
        join_kernel,
        in_specs=[pl.BlockSpec(memory_space=pltpu.SMEM), vmem, vmem],
        out_specs=vmem,
        out_shape=jax.ShapeDtypeStruct(received.shape[::-1], f32),
        cost_estimate=pl.CostEstimate(
            flops=1_000_000_000, bytes_accessed=4_000_000, transcendentals=0
        ),
        name="join",
    )(core.reshape(1), products, received)


def exchange(pieces, axis, groups=None):
    return lax.all_to_all(pieces, axis, 0, 0, axis_index_groups=groups)


def gather(piece, axis, count, groups=None):
    return exchange(jnp.broadcast_to(piece, (count, *piece.shape)), axis, groups)


def per_device(matrix):
    my_row, my_col = lax.axis_index("prow"), lax.axis_index("pcol")
    rows_count, cols_count = lax.axis_size("prow"), lax.axis_size("pcol")
    core, level = my_row % CORES, my_row // CORES
    on_top, has_panel = my_row == 0, my_col == 0
    levels = [[CORES * z + c for z in range(LEVELS)] for c in range(CORES)]
    rows, cols = matrix.shape
    high = lax.Precision.HIGH

    def permute(value, pairs):
        return lax.ppermute(value, "prow", pairs)

    def swap(value):
        return permute(value, [(i, i ^ 1) for i in range(rows_count)])

    column_ids = lax.broadcasted_iota(jnp.int32, (1, cols), 1)
    replaced = has_panel & (column_ids < WIDE)
    pieces = matrix[:, :WIDE].reshape(cols_count, -1, WIDE)
    panel_piece = exchange(pieces, "pcol")[0]
    low, high_half = jnp.split(matrix[:WIDE].T, CORES)
    panel = gather(panel_piece, "pcol", cols_count).reshape(rows, WIDE)

    top_half = jnp.where(core == 0, low, permute(high_half, [(0, 1)]))
    held = top_half.reshape(LEVELS, -1, WIDE)
    step = LEVELS // 2
    while step:
        givers = range(0, LEVELS, 2 * step)
        pairs = [(CORES * z + c, CORES * (z + step) + c) for z in givers for c in range(CORES)]
        received = permute(held[step:], pairs)
        held = jnp.where(level % (2 * step) == 0, held[:step], received)
        step //= 2
    panel, top_slice = lax.optimization_barrier((panel, held[0]))

    strip = WIDE // cols_count
    squares = [
        lax.dynamic_slice_in_dim(a, my_col * strip, strip, 0)
        for a in (transposed_product(panel, panel), panel)
    ]
    squares = jnp.concatenate([squares[0], jnp.where(on_top, squares[1], 0.0)], axis=0)
    squares, panel = lax.optimization_barrier((squares + swap(squares), panel))
    squares = gather(squares, "prow", LEVELS, levels)
    products = transposed_product(panel, matrix, high)
    low_half, high_half = jnp.split(products, CORES, axis=1)
    other = jnp.where(core == 0, high_half, low_half)
    squares = gather(squares.sum(0), "pcol", cols_count)
    base = lax.optimization_barrier(jnp.where(replaced, 0.0, matrix))
    mine = joined(core, products, swap(other))
    squares, mine = lax.optimization_barrier((squares, mine))
    summed = exchange(mine.reshape(LEVELS, -1, WIDE), "prow", levels)
    gram, top = (a.reshape(WIDE, WIDE) for a in jnp.split(squares, 2, axis=1))
    summed = summed.sum(0)
    upper, inverse = cholesky(gram)
    summed = summed + product(top_slice, upper)
    summed = gather(summed, "prow", LEVELS, levels).reshape(-1, WIDE)
    square, factors, panel_weights = lower_upper(top, upper, inverse)
    shifted = jnp.concatenate(
        [jnp.where(on_top, panel[:WIDE] + upper, panel[:WIDE]), panel[WIDE:]], axis=0
    )
    above = jnp.triu(jnp.ones((WIDE, WIDE), jnp.bool_))
    corner = jnp.where(above, -upper - jnp.eye(WIDE, dtype=f32), 0.0)
    corner = jnp.where(on_top & has_panel, corner, base[:WIDE, :WIDE])
    base = base.at[:WIDE, :WIDE].set(corner)
    sibling = swap(summed)
    mine, other = (
        lax.dot_general(
            square, a, (((1,), (1,)), ((), ())), precision=high, preferred_element_type=f32
        )
        for a in (summed, sibling)
    )
    weights = jnp.where(
        core == 0,
        jnp.concatenate([mine, other], axis=1),
        jnp.concatenate([other, mine], axis=1),
    )
    weights = weights.at[:, :WIDE].set(jnp.where(has_panel, panel_weights, weights[:, :WIDE]))
    return (base - product(shifted, weights, high), factors)


def solution(mesh):
    placed = (P("prow", "pcol"),)
    return jax.shard_map(
        per_device, mesh=mesh, in_specs=placed, out_specs=(P("prow", "pcol"), P()), check_vma=False
    )
```

```python
import jax
import jax.numpy as jnp
from jax import lax
from jax.experimental import pallas as pl
from jax.experimental.pallas import tpu as pltpu
from jax.sharding import PartitionSpec as P


NB = 128
WIDE = 2 * NB
STRIP = 8
LEVELS, CORES = 8, 2

f32, bf16 = jnp.float32, jnp.bfloat16


def three_parts(value):
    first = value.astype(bf16).astype(f32)
    rest = value - first
    second = rest.astype(bf16).astype(f32)
    return first, second, (rest - second).astype(bf16).astype(f32)


def strip_product(left, right):
    a, b, c = three_parts(left)
    d, e, f = three_parts(right)
    return lax.dot_general(
        jnp.concatenate([a, a, b, b, a, c], axis=0).astype(bf16),
        jnp.concatenate([d, e, d, e, f, d], axis=0).astype(bf16),
        (((0,), (0,)), ((), ())),
        preferred_element_type=f32,
    )


def strip_columns(rows, first, lanes):
    return [
        jnp.sum(jnp.where(lanes == first + c, rows, 0.0), axis=1, keepdims=True)
        for c in range(STRIP)
    ]


def identity_matrix():
    rows = lax.broadcasted_iota(jnp.int32, (WIDE, WIDE), 0)
    return (rows == lax.broadcasted_iota(jnp.int32, (WIDE, WIDE), 1)).astype(f32)


def strips_of(half):
    count = WIDE // STRIP // 2
    return half * count, (half + 1) * count


def cholesky_kernel(gram_ref, upper_ref, inverse_ref, work):
    work[:, :WIDE] = gram_ref[...]
    work[:, WIDE:] = identity_matrix()
    lanes = lax.broadcasted_iota(jnp.int32, (STRIP, WIDE), 1)
    row_ids = lax.broadcasted_iota(jnp.int32, (STRIP, WIDE), 0)
    sub_narrow = lax.broadcasted_iota(jnp.int32, (STRIP, 1), 0)
    sub_wide = lax.broadcasted_iota(jnp.int32, (STRIP, 2 * WIDE), 0)
    for half in range(2):
        low, high = half * NB, half * NB + 3 * NB

        def strip(index, carry):
            first = pl.multiple_of(index * STRIP, STRIP)
            rows = work[pl.ds(first, STRIP), :]
            diag = strip_columns(rows[:, :WIDE], first, lanes)
            for c in range(STRIP):
                inverse = lax.rsqrt(diag[c][c : c + 1])
                pivot_row = rows[c : c + 1] * inverse
                factor = jnp.where(sub_narrow > c, diag[c] * inverse, 0.0)
                for d in range(c + 1, STRIP):
                    diag[d] = diag[d] - factor * (diag[d][c : c + 1] * inverse)
                rows = jnp.where(sub_wide == c, pivot_row, rows - factor * pivot_row)
            upper_ref[pl.ds(first, STRIP), :] = jnp.where(
                lanes >= first + row_ids, rows[:, :WIDE], 0.0
            )
            inverse_ref[pl.ds(first, STRIP), :] = rows[:, WIDE:]
            left = jnp.where(lanes >= first + STRIP, rows[:, :WIDE], 0.0)[:, low:]
            work[low:, low:high] = work[low:, low:high] - strip_product(left, rows[:, low:high])
            return carry

        lax.fori_loop(*strips_of(half), strip, 0)


def sharp_product(left, right, right_turned=False):
    a, b, c = three_parts(left)
    d, e, f = three_parts(right)
    axis = 1 if right_turned else 0
    return lax.dot_general(
        jnp.concatenate([a, a, b, b, a, c], axis=1).astype(bf16),
        jnp.concatenate([d, e, d, e, f, d], axis=axis).astype(bf16),
        (((1,), (axis,)), ((), ())),
        preferred_element_type=f32,
    )


def lower_upper_kernel(
    top_ref, r_ref, inverse_ref, square_ref, factors_ref, panel_ref, work, turned_work
):
    total = top_ref[...] + r_ref[...]
    work[:, :WIDE] = total
    work[:, WIDE:] = identity_matrix()
    turned_work[:, :WIDE] = total.T
    turned_work[:, WIDE:] = identity_matrix()
    lanes = lax.broadcasted_iota(jnp.int32, (STRIP, WIDE), 1)
    row_ids = lax.broadcasted_iota(jnp.int32, (STRIP, WIDE), 0)
    sub_narrow = lax.broadcasted_iota(jnp.int32, (STRIP, 1), 0)
    sub_wide = lax.broadcasted_iota(jnp.int32, (STRIP, 2 * WIDE), 0)
    for half in range(2):
        low, high = half * NB, half * NB + 3 * NB

        def strip(index, carry):
            first = pl.multiple_of(index * STRIP, STRIP)
            rows = work[pl.ds(first, STRIP), :]
            turned = turned_work[pl.ds(first, STRIP), :]
            diag = strip_columns(rows[:, :WIDE], first, lanes)
            diag_turned = strip_columns(turned[:, :WIDE], first, lanes)
            for c in range(STRIP):
                inverse = 1.0 / diag[c][c : c + 1]
                factor = jnp.where(sub_narrow > c, diag[c] * inverse, 0.0)
                factor_turned = jnp.where(sub_narrow > c, diag_turned[c], 0.0)
                for d in range(c + 1, STRIP):
                    diag[d] = diag[d] - factor * diag[d][c : c + 1]
                    diag_turned[d] = diag_turned[d] - factor_turned * (
                        diag_turned[d][c : c + 1] * inverse
                    )
                rows = rows - factor * rows[c : c + 1]
                pivot_row = turned[c : c + 1] * inverse
                turned = jnp.where(sub_wide == c, pivot_row, turned - factor_turned * pivot_row)
            after = lanes >= first + STRIP
            left = jnp.where(after, rows[:, :WIDE], 0.0)[:, low:]
            left_turned = jnp.where(after, turned[:, :WIDE], 0.0)[:, low:]
            work[low:, low:high] = work[low:, low:high] - strip_product(
                left_turned, rows[:, low:high]
            )
            turned_work[low:, low:high] = turned_work[low:, low:high] - strip_product(
                left, turned[:, low:high]
            )
            kept = lanes >= first + row_ids
            work[pl.ds(first, STRIP), :WIDE] = jnp.where(kept, rows[:, :WIDE], 0.0)
            work[pl.ds(first, STRIP), WIDE:] = rows[:, WIDE:]
            turned_work[pl.ds(first, STRIP), WIDE:] = turned[:, WIDE:]
            return carry

        lax.fori_loop(*strips_of(half), strip, 0)
    inner = sharp_product(work[:, WIDE:], inverse_ref[...])
    upper_inv = turned_work[:, WIDE:].T
    square_ref[...] = sharp_product(upper_inv, inner)
    panel_ref[...] = -upper_inv
    for k in range(2):
        block = slice(k * NB, (k + 1) * NB)
        factors_ref[k] = sharp_product(work[block, block], inner[block, block], right_turned=True)


square_shape = jax.ShapeDtypeStruct((WIDE, WIDE), f32)


def cholesky(gram):
    return pl.pallas_call(
        cholesky_kernel,
        out_shape=(square_shape,) * 2,
        scratch_shapes=[pltpu.VMEM((WIDE, 2 * WIDE), f32)],
        cost_estimate=pl.CostEstimate(
            flops=14_000_000_000, bytes_accessed=800_000, transcendentals=0
        ),
        name="cholesky",
    )(gram)


def lower_upper(top, r, inverse):
    return pl.pallas_call(
        lower_upper_kernel,
        out_shape=(square_shape, jax.ShapeDtypeStruct((2, NB, NB), f32), square_shape),
        scratch_shapes=[pltpu.VMEM((WIDE, 2 * WIDE), f32)] * 2,
        cost_estimate=pl.CostEstimate(
            flops=17_000_000_000, bytes_accessed=1_600_000, transcendentals=0
        ),
        name="lower_upper",
    )(top, r, inverse)


def product(left, right, precision=lax.Precision.HIGHEST):
    return jnp.dot(left, right, precision=precision, preferred_element_type=f32)


def transposed_product(left, right, precision=lax.Precision.HIGHEST):
    return lax.dot_general(
        left, right, (((0,), (0,)), ((), ())), precision=precision, preferred_element_type=f32
    )


def join_kernel(flags, products_ref, received_ref, joined_ref):
    width = received_ref.shape[1]
    half = jnp.where(flags[0] == 0, products_ref[:, :width], products_ref[:, width:])
    joined_ref[...] = (half + received_ref[...]).T


def joined(core, products, received):
    vmem = pl.BlockSpec(memory_space=pltpu.VMEM)
    return pl.pallas_call(
        join_kernel,
        in_specs=[pl.BlockSpec(memory_space=pltpu.SMEM), vmem, vmem],
        out_specs=vmem,
        out_shape=jax.ShapeDtypeStruct(received.shape[::-1], f32),
        cost_estimate=pl.CostEstimate(
            flops=1_000_000_000, bytes_accessed=4_000_000, transcendentals=0
        ),
        name="join",
    )(core.reshape(1), products, received)


def exchange(pieces, axis, groups=None):
    return lax.all_to_all(pieces, axis, 0, 0, axis_index_groups=groups)


def gather(piece, axis, count, groups=None):
    return exchange(jnp.broadcast_to(piece, (count, *piece.shape)), axis, groups)


def per_device(matrix):
    my_row, my_col = lax.axis_index("prow"), lax.axis_index("pcol")
    rows_count, cols_count = lax.axis_size("prow"), lax.axis_size("pcol")
    core, level = my_row % CORES, my_row // CORES
    on_top, has_panel = my_row == 0, my_col == 0
    levels = [[CORES * z + c for z in range(LEVELS)] for c in range(CORES)]
    rows, cols = matrix.shape
    high, highest = lax.Precision.HIGH, lax.Precision.HIGHEST

    def permute(value, pairs):
        return lax.ppermute(value, "prow", pairs)

    def swap(value):
        return permute(value, [(i, i ^ 1) for i in range(rows_count)])

    column_ids = lax.broadcasted_iota(jnp.int32, (1, cols), 1)
    replaced = has_panel & (column_ids < WIDE)
    pieces = matrix[:, :WIDE].reshape(cols_count, -1, WIDE)
    panel_piece = exchange(pieces, "pcol")[0]
    low, high_half = jnp.split(matrix[:WIDE].T, CORES)
    panel = gather(panel_piece, "pcol", cols_count).reshape(rows, WIDE)

    top_half = jnp.where(core == 0, low, permute(high_half, [(0, 1)]))
    held = top_half.reshape(LEVELS, -1, WIDE)
    step = LEVELS // 2
    while step:
        givers = range(0, LEVELS, 2 * step)
        pairs = [(CORES * z + c, CORES * (z + step) + c) for z in givers for c in range(CORES)]
        received = permute(held[step:], pairs)
        held = jnp.where(level % (2 * step) == 0, held[:step], received)
        step //= 2
    panel, top_slice = lax.optimization_barrier((panel, held[0]))

    strip = WIDE // cols_count
    squares = [
        lax.dynamic_slice_in_dim(a, my_col * strip, strip, 0)
        for a in (transposed_product(panel, panel), panel)
    ]
    squares = jnp.concatenate([squares[0], jnp.where(on_top, squares[1], 0.0)], axis=0)
    squares, panel = lax.optimization_barrier((squares + swap(squares), panel))
    squares = gather(squares, "prow", LEVELS, levels)
    products = transposed_product(panel, matrix)
    low_half, high_half = jnp.split(products, CORES, axis=1)
    other = jnp.where(core == 0, high_half, low_half)
    squares = gather(squares.sum(0), "pcol", cols_count)
    base = lax.optimization_barrier(jnp.where(replaced, 0.0, matrix))
    mine = joined(core, products, swap(other))
    squares, mine = lax.optimization_barrier((squares, mine))
    summed = exchange(mine.reshape(LEVELS, -1, WIDE), "prow", levels)
    gram, top = (a.reshape(WIDE, WIDE) for a in jnp.split(squares, 2, axis=1))
    summed = summed.sum(0)
    upper, inverse = cholesky(gram)
    summed = summed + product(top_slice, upper)
    summed = gather(summed, "prow", LEVELS, levels).reshape(-1, WIDE)
    square, factors, panel_weights = lower_upper(top, upper, inverse)
    shifted = jnp.concatenate(
        [jnp.where(on_top, panel[:WIDE] + upper, panel[:WIDE]), panel[WIDE:]], axis=0
    )
    above = jnp.triu(jnp.ones((WIDE, WIDE), jnp.bool_))
    corner = jnp.where(above, -upper - jnp.eye(WIDE, dtype=f32), 0.0)
    corner = jnp.where(on_top & has_panel, corner, base[:WIDE, :WIDE])
    base = base.at[:WIDE, :WIDE].set(corner)
    sibling = swap(summed)
    mine, other = (
        lax.dot_general(
            square, a, (((1,), (1,)), ((), ())), precision=highest, preferred_element_type=f32
        )
        for a in (summed, sibling)
    )
    weights = jnp.where(
        core == 0,
        jnp.concatenate([mine, other], axis=1),
        jnp.concatenate([other, mine], axis=1),
    )
    weights = weights.at[:, :WIDE].set(jnp.where(has_panel, panel_weights, weights[:, :WIDE]))
    return (base - product(shifted, weights, high), factors)


def solution(mesh):
    placed = (P("prow", "pcol"),)
    return jax.shard_map(
        per_device, mesh=mesh, in_specs=placed, out_specs=(P("prow", "pcol"), P()), check_vma=False
    )
```
